32 devices in a mesh: slab: 4 (over x, core), img: 8 (over z, y).
Axes of the slice: x: 2, y: 2, z: 4, core: 2. Of those that a mesh axis runs over, the one named last changes fastest.
Arguments:
- feats: bfloat16 [8, 32, 128, 512], P('img', 'slab'), may hold values from -6 to 6
- labels: int32 [8], P('img'), may hold values from 0 to 999
- conv_w: bfloat16 [9, 512, 4], replicated, may hold values from -0.09375 to 0.09375
- embed_w: bfloat16 [16, 1024], replicated, may hold values from -1.5 to 1.5
- mod_table: bfloat16 [1000, 2048], replicated, may hold values from -3 to 3
- qkv_w: bfloat16 [1024, 3072], replicated, may hold values from -0.1875 to 0.1875
- out_w: bfloat16 [1024, 1024], replicated, may hold values from -0.1875 to 0.1875
- proj_w: bfloat16 [1024, 768], replicated, may hold values from -0.1875 to 0.1875
- dino: bfloat16 [8, 1024, 768], P('img', 'slab'), may hold values from -6 to 6
Outputs:
- grad_feats: bfloat16 [8, 32, 128, 512], P('img', 'slab')
- grad_proj: float32 [1024, 768], replicated
- grad_conv: float32 [9, 512, 4], replicated
- loss: float32 [], replicated
The draws below stay inside these ranges and needn't reach their ends.
All inputs are finite; a program needn't handle non-finite values.
Results may differ from the reference program's by a relative error of at most 0.024.
Values may be sent and summed in bfloat16 or wider, within the bound.
A program may use at most 128 MiB of HBM per device.

```python
import jax
import jax.numpy as jnp
from jax import lax

C = 512
LAT = 4
D = 1024
HEAD_DIM = 64
DINO = 768
CLASSES = 1000
WL = 128
HL = 32
TOK_IMG = 1024
IMAGES = 8


def place_ends(drawn, own_key, low, high):
    extent = drawn.shape
    spot = [jax.random.randint(jax.random.fold_in(own_key, axis), (), 0, extent[axis]) for axis in range(len(extent))]
    drawn = drawn.at[tuple(spot)].set(low)
    longest = extent.index(max(extent))
    spot[longest] = (spot[longest] + 1) % extent[longest]
    return drawn.at[tuple(spot)].set(high)


def levels(own_key, shape, split, smallest, high):
    def one(position, blocks):
        draws = jax.random.uniform(jax.random.fold_in(jax.random.fold_in(own_key, 6), position), (blocks,), jnp.float32, smallest / len(split), high / len(split))
        return jnp.repeat(jnp.exp(draws), shape[position] // blocks).reshape((-1,) + (1,) * (len(shape) - position - 1))

    factor_of = one(*split[0])
    for cut in split[1:]:
        factor_of = factor_of * one(*cut)
    return factor_of


def centred(key, extent, scale, reach, shards=(), kind=jnp.bfloat16):
    values = scale * jax.random.normal(key, extent, jnp.float32)
    if shards:
        values = values * levels(key, extent, shards, -0.22, 0.18)
    return jnp.clip(values, -reach, reach).astype(kind)


def setup_inputs(seed: int = 0) -> dict:
    keys = jax.random.split(jax.random.key(seed), 10)
    return {
        "feats": centred(keys[0], (IMAGES, HL, WL, C), 1.0, 6.0, ((0, 8), (1, 4))),
        "labels": place_ends(jax.random.randint(keys[1], (IMAGES,), 0, CLASSES), jax.random.fold_in(keys[1], 1), 0, CLASSES - 1).astype(jnp.int32),
        "conv_w": centred(keys[2], (9, C, LAT), (9 * C) ** -0.5, 0.09375),
        "embed_w": centred(keys[3], (4 * LAT, D), (4 * LAT) ** -0.5, 1.5),
        "mod_table": centred(keys[4], (CLASSES, 2 * D), 0.5, 3.0),
        "qkv_w": centred(keys[5], (D, 3 * D), D ** -0.5, 0.1875),
        "out_w": centred(keys[6], (D, D), D ** -0.5, 0.1875),
        "proj_w": centred(keys[7], (D, DINO), D ** -0.5, 0.1875),
        "dino": centred(keys[8], (IMAGES, TOK_IMG, DINO), 1.0, 6.0, ((0, 8), (1, 4))),
    }


latent_scale = 0.18215
norm_eps = 1e-06
cosine_eps = 1e-06

def conv_out(padded, conv_w):
    rows = padded.shape[0] - 2
    cols = padded.shape[1] - 2
    total = jnp.zeros((rows * cols, conv_w.shape[2]), jnp.float32)
    for tap in range(9):
        view = padded[tap // 3:tap // 3 + rows, tap % 3:tap % 3 + cols]
        total = total + jnp.dot(view.reshape(rows * cols, -1), conv_w[tap], preferred_element_type=jnp.float32)
    return total.reshape(rows, cols, -1) * latent_scale

def conv_back(padded, grad_pad, conv_w):
    rows = grad_pad.shape[0] - 2
    cols = grad_pad.shape[1] - 2
    center = grad_pad[1:-1, 1:-1].reshape(rows * cols, -1)
    grad_in = jnp.zeros((rows * cols, conv_w.shape[1]), jnp.float32)
    parts = []
    for tap in range(9):
        row_off = tap // 3
        col_off = tap % 3
        g_view = grad_pad[2 - row_off:2 - row_off + rows, 2 - col_off:2 - col_off + cols].reshape(rows * cols, -1)
        grad_in = grad_in + jnp.dot(g_view, conv_w[tap].T, preferred_element_type=jnp.float32)
        f_view = padded[row_off:row_off + rows, col_off:col_off + cols].reshape(rows * cols, -1)
        parts.append(jnp.dot(f_view.T, center, preferred_element_type=jnp.float32))
    return (grad_in.reshape(rows, cols, -1), jnp.stack(parts, 0))

def patchify(latent):
    rows, cols, chans = latent.shape
    blocks = latent.reshape(rows // 2, 2, cols // 2, 2, chans).transpose(0, 2, 1, 3, 4)
    return blocks.reshape(rows // 2 * (cols // 2), 4 * chans)

def unpatchify(tokens, rows, cols):
    chans = tokens.shape[1] // 4
    blocks = tokens.reshape(rows // 2, cols // 2, 2, 2, chans).transpose(0, 2, 1, 3, 4)
    return blocks.reshape(rows, cols, chans)

def cosine_grad(projected, target):
    norm_p = jnp.sqrt(lax.optimization_barrier(jnp.sum(projected * projected, -1, keepdims=True)) + cosine_eps)
    norm_t = jnp.sqrt(lax.optimization_barrier(jnp.sum(target * target, -1, keepdims=True)) + cosine_eps)
    cosine = lax.optimization_barrier(jnp.sum(projected * target, -1, keepdims=True)) / (norm_p * norm_t)
    grad = cosine * projected / (norm_p * norm_p) - target / (norm_p * norm_t)
    return (cosine[:, 0], grad)

def widen(x):
    return lax.optimization_barrier(x.astype(jnp.bfloat16)).astype(jnp.float32)

def one_image(image, label, target_b, conv_w, embed_w, mod_table, qkv_w, out_w, proj_w):
    rows, cols, chans = image.shape
    width = qkv_w.shape[0]
    heads = width // HEAD_DIM
    scale = HEAD_DIM ** (-0.5)
    padded = jnp.pad(image, ((1, 1), (1, 1), (0, 0)))
    tokens = patchify(conv_out(padded, conv_w))
    count = tokens.shape[0]
    embed_f = embed_w.astype(jnp.float32)
    start = jnp.dot(tokens, embed_f, precision=lax.Precision.HIGHEST)
    row = mod_table[label].astype(jnp.float32)
    mean = lax.optimization_barrier(jnp.mean(start, -1, keepdims=True))
    cent = start - mean
    inv = lax.rsqrt(lax.optimization_barrier(jnp.mean(cent * cent, -1, keepdims=True)) + norm_eps)
    normed = cent * inv
    modded = (normed * (1.0 + row[width:]) + row[:width]).astype(jnp.bfloat16)
    qkv = jnp.dot(modded, qkv_w, preferred_element_type=jnp.float32).astype(jnp.bfloat16)
    q3 = qkv[:, :width].astype(jnp.float32).reshape(count, heads, HEAD_DIM)
    k3 = qkv[:, width:2 * width].astype(jnp.float32).reshape(count, heads, HEAD_DIM)
    v3 = qkv[:, 2 * width:].astype(jnp.float32).reshape(count, heads, HEAD_DIM)
    scores = jnp.einsum('qhd,khd->hqk', q3, k3) * scale
    top = lax.optimization_barrier(jnp.max(scores, -1, keepdims=True))
    expo = jnp.exp(scores - top)
    total = lax.optimization_barrier(jnp.sum(expo, -1))
    attended = jnp.einsum('hqk,khd->qhd', widen(expo), v3) / total.T[:, :, None]
    attended = attended.reshape(count, width).astype(jnp.bfloat16)
    lse = top[..., 0] + jnp.log(total)
    resid = start + jnp.dot(attended, out_w, preferred_element_type=jnp.float32)
    resid_b = resid.astype(jnp.bfloat16)
    projected = jnp.dot(resid_b, proj_w, preferred_element_type=jnp.float32)
    cosine, grad_p = cosine_grad(projected, target_b.astype(jnp.float32))
    grad_pb = grad_p.astype(jnp.bfloat16)
    proj_part = jnp.dot(resid_b.T, grad_pb, preferred_element_type=jnp.float32)
    grad_resid = jnp.dot(grad_pb, proj_w.T, preferred_element_type=jnp.float32)
    grad_att = jnp.dot(grad_resid.astype(jnp.bfloat16), out_w.T, preferred_element_type=jnp.float32).astype(jnp.bfloat16)
    g3 = grad_att.astype(jnp.float32).reshape(count, heads, HEAD_DIM)
    delta = lax.optimization_barrier(jnp.sum(g3 * attended.astype(jnp.float32).reshape(count, heads, HEAD_DIM), -1)).T
    probs = jnp.exp(scores - lse[..., None])
    dprobs = jnp.einsum('qhd,khd->hqk', g3, v3)
    dscores = widen(probs * (dprobs - delta[..., None]))
    grad_q = scale * jnp.einsum('hqk,khd->qhd', dscores, k3).reshape(count, width)
    grad_k = scale * jnp.einsum('hqk,qhd->khd', dscores, q3).reshape(count, width)
    grad_v = jnp.einsum('hqk,qhd->khd', widen(probs), g3).reshape(count, width)
    grad_qkv = jnp.concatenate([grad_q, grad_k, grad_v], 1).astype(jnp.bfloat16)
    grad_mod = jnp.dot(grad_qkv, qkv_w.T, preferred_element_type=jnp.float32)
    grad_norm = grad_mod * (1.0 + row[width:])
    grad_start = grad_resid + inv * (grad_norm - lax.optimization_barrier(jnp.mean(grad_norm, -1, keepdims=True)) - normed * lax.optimization_barrier(jnp.mean(grad_norm * normed, -1, keepdims=True)))
    grad_tokens = jnp.dot(grad_start, embed_f.T, precision=lax.Precision.HIGHEST)
    grad_latent = (unpatchify(grad_tokens, rows, cols) * latent_scale).astype(jnp.bfloat16)
    grad_pad = jnp.pad(grad_latent, ((1, 1), (1, 1), (0, 0)))
    grad_image, conv_part = conv_back(padded, grad_pad, conv_w)
    return (grad_image.astype(jnp.bfloat16), proj_part, conv_part, jnp.sum(1.0 - cosine))

def reference(feats, labels, conv_w, embed_w, mod_table, qkv_w, out_w, proj_w, dino):

    def step(args):
        image, label, target = args
        return one_image(image, label, target, conv_w, embed_w, mod_table, qkv_w, out_w, proj_w)
    grads, proj_parts, conv_parts, losses = lax.map(step, (feats, labels, dino))
    loss = jnp.sum(losses) / (IMAGES * TOK_IMG)
    return (grads, lax.optimization_barrier(jnp.sum(proj_parts, 0)), lax.optimization_barrier(jnp.sum(conv_parts, 0)), loss)
```

```python
import functools
import math

import jax
import jax.numpy as jnp
from jax import lax
from jax.experimental import pallas as pl
from jax.experimental.pallas import tpu as pltpu
from jax.sharding import PartitionSpec as P

HEAD_DIM = 64
PAIR = 2 * HEAD_DIM

latent_scale = 0.18215
norm_eps = 1e-06
cosine_eps = 1e-06

MESH_ID = pl.DeviceIdType.MESH


def mm(left, right, dims, kind=jnp.float32):
    return lax.dot_general(left, right, (dims, ((), ())), preferred_element_type=kind)


def contract_first(left, right):
    return mm(left, right, ((0,), (0,)))


def contract_last(left, right):
    return mm(left, right, ((1,), (1,)))


def attend_kernel(q_ref, k_ref, v_ref, o_ref, lse_ref):
    scale = HEAD_DIM ** (-0.5)
    outs = []
    for h in range(2):
        cut = slice(h * HEAD_DIM, (h + 1) * HEAD_DIM)
        s = contract_last(k_ref[:, cut], q_ref[:, cut] * jnp.bfloat16(scale))
        top = jnp.max(s, 0, keepdims=True)
        e = jnp.exp(s - top)
        total = jnp.sum(e, 0, keepdims=True)
        o = contract_first(v_ref[:, cut], e.astype(jnp.bfloat16)) / total
        lse_ref[0, h : h + 1, :] = top + jnp.log(total)
        outs.append(o)
    o_ref[...] = jnp.concatenate(outs, 0).T.astype(jnp.bfloat16)


def attend_back_kernel(q_ref, k_ref, v_ref, g_ref, o_ref, lse_ref, gq_ref, gk_ref, gv_ref):
    scale = HEAD_DIM ** (-0.5)
    prod = (g_ref[...].astype(jnp.float32) * o_ref[...].astype(jnp.float32)).T
    gqs = []
    for h in range(2):
        cut = slice(h * HEAD_DIM, (h + 1) * HEAD_DIM)
        qs = q_ref[:, cut] * jnp.bfloat16(scale)
        k = k_ref[:, cut]
        g = g_ref[:, cut]
        delta = jnp.sum(prod[cut], 0, keepdims=True)
        p = jnp.exp(contract_last(k, qs) - lse_ref[0, h : h + 1, :])
        ds = (p * (contract_last(v_ref[:, cut], g) - delta)).astype(jnp.bfloat16)
        gk_ref[:, cut] = mm(ds, qs, ((1,), (0,))).astype(jnp.bfloat16)
        gv_ref[:, cut] = mm(p.astype(jnp.bfloat16), g, ((1,), (0,))).astype(jnp.bfloat16)
        gqs.append(contract_first(k, ds) * scale)
    gq_ref[...] = jnp.concatenate(gqs, 0).T.astype(jnp.bfloat16)


def attend(query, kv):
    count, width = query.shape
    full = kv.shape[0]
    pairs = width // PAIR
    cost = pl.CostEstimate(
        flops=4 * count * full * width, bytes_accessed=2 * (2 * full + 2 * count) * width,
        transcendentals=count * full * width // HEAD_DIM)
    return pl.pallas_call(
        attend_kernel,
        grid=(pairs,),
        in_specs=[
            pl.BlockSpec((count, PAIR), lambda i: (0, i)),
            pl.BlockSpec((full, PAIR), lambda i: (0, i)),
            pl.BlockSpec((full, PAIR), lambda i: (0, i + pairs)),
        ],
        out_specs=[
            pl.BlockSpec((count, PAIR), lambda i: (0, i)),
            pl.BlockSpec((1, 2, count), lambda i: (i, 0, 0)),
        ],
        out_shape=[
            jax.ShapeDtypeStruct((count, width), jnp.bfloat16),
            jax.ShapeDtypeStruct((pairs, 2, count), jnp.float32),
        ],
        cost_estimate=cost,
        name="attend",
    )(query, kv, kv)


def attend_back(query, kv, grad, attended, lse):
    count, width = query.shape
    full = kv.shape[0]
    pairs = width // PAIR
    cost = pl.CostEstimate(
        flops=10 * count * full * width, bytes_accessed=2 * (4 * full + 4 * count) * width,
        transcendentals=count * full * width // HEAD_DIM)
    small = pl.BlockSpec((count, PAIR), lambda i: (0, i))
    large = pl.BlockSpec((full, PAIR), lambda i: (0, i))
    return pl.pallas_call(
        attend_back_kernel,
        grid=(pairs,),
        in_specs=[
            small,
            large,
            pl.BlockSpec((full, PAIR), lambda i: (0, i + pairs)),
            small,
            small,
            pl.BlockSpec((1, 2, count), lambda i: (i, 0, 0)),
        ],
        out_specs=[small, large, large],
        out_shape=[
            jax.ShapeDtypeStruct((count, width), jnp.bfloat16),
            jax.ShapeDtypeStruct((full, width), jnp.bfloat16),
            jax.ShapeDtypeStruct((full, width), jnp.bfloat16),
        ],
        cost_estimate=cost,
        name="attend_back",
    )(query, kv, kv, grad, attended, lse)


def reduce_kernel(slabs, images, x_ref, out_ref, recv, send1, recv1, send2, recv2):
    count = slabs * images
    me = lax.axis_index("slab") * images + lax.axis_index("img")

    def where(step):
        peer = lax.rem(me + step, count)
        return peer, {"slab": peer // images, "img": lax.rem(peer, images)}

    barrier = pltpu.get_barrier_semaphore()

    def hello(step, _):
        _, spot = where(step)
        pl.semaphore_signal(barrier, inc=1, device_id=spot, device_id_type=MESH_ID)
        return 0

    lax.fori_loop(1, count, hello, 0)
    pl.semaphore_wait(barrier, count - 1)

    def spread(step):
        peer, spot = where(step)
        return pltpu.make_async_remote_copy(
            src_ref=x_ref.at[peer], dst_ref=recv.at[me], send_sem=send1.at[peer],
            recv_sem=recv1.at[me], device_id=spot, device_id_type=MESH_ID)

    def arrive(step):
        peer, spot = where(step)
        return pltpu.make_async_remote_copy(
            src_ref=x_ref.at[peer], dst_ref=recv.at[peer], send_sem=send1.at[peer],
            recv_sem=recv1.at[peer], device_id=spot, device_id_type=MESH_ID)

    def share(step):
        peer, spot = where(step)
        return pltpu.make_async_remote_copy(
            src_ref=out_ref.at[me], dst_ref=out_ref.at[me], send_sem=send2.at[peer],
            recv_sem=recv2.at[me], device_id=spot, device_id_type=MESH_ID)

    def landed(step):
        peer, spot = where(step)
        return pltpu.make_async_remote_copy(
            src_ref=out_ref.at[me], dst_ref=out_ref.at[peer], send_sem=send2.at[peer],
            recv_sem=recv2.at[peer], device_id=spot, device_id_type=MESH_ID)

    def each(body):
        def run(step, _):
            body(step)
            return 0

        lax.fori_loop(1, count, run, 0)

    each(lambda step: spread(step).start())
    each(lambda step: arrive(step).wait_recv())
    total = x_ref[me]
    total = lax.fori_loop(
        1, count, lambda step, acc: acc + recv[lax.rem(me + step, count)], total)
    out_ref[me] = total
    each(lambda step: share(step).start())
    each(lambda step: spread(step).wait_send())
    each(lambda step: landed(step).wait_recv())
    each(lambda step: share(step).wait_send())


def reduce_small(flat, slabs, images):
    count = slabs * images
    rows = math.ceil(flat.size / count / 1024) * 8
    cells = jnp.pad(flat, (0, count * rows * 128 - flat.size)).reshape(count, rows, 128)
    vmem = pl.BlockSpec(memory_space=pltpu.VMEM)
    out = pl.pallas_call(
        functools.partial(reduce_kernel, slabs, images),
        out_shape=jax.ShapeDtypeStruct(cells.shape, cells.dtype),
        in_specs=[vmem],
        out_specs=vmem,
        scratch_shapes=[pltpu.VMEM(cells.shape, cells.dtype)]
        + [pltpu.SemaphoreType.DMA((count,))] * 4,
        compiler_params=pltpu.CompilerParams(collective_id=0, has_side_effects=True),
        name="reduce_small",
    )(cells)
    return out.reshape(-1)[: flat.size]


def cosine_grad(projected, target):
    norm_p = jnp.sqrt(jnp.sum(projected * projected, -1, keepdims=True) + cosine_eps)
    norm_t = jnp.sqrt(jnp.sum(target * target, -1, keepdims=True) + cosine_eps)
    cosine = jnp.sum(projected * target, -1, keepdims=True) / (norm_p * norm_t)
    grad = cosine * projected / (norm_p * norm_p) - target / (norm_p * norm_t)
    return (cosine[:, 0], grad)


def local(feats, labels, conv_w, embed_w, mod_table, qkv_w, out_w, proj_w, dino):
    image = feats[0]
    rows, cols, chans = image.shape
    outs = conv_w.shape[2]
    width = qkv_w.shape[0]
    slabs = lax.axis_size("slab")
    images = lax.axis_size("img")
    slab = lax.axis_index("slab")
    cells = image.reshape(rows * cols, chans)
    taps = conv_w.transpose(0, 2, 1).reshape(9 * outs, chans)
    resp = contract_last(taps, cells).reshape(3, 3, outs, rows, cols)
    resp = jnp.pad(resp, ((0, 0), (0, 0), (0, 0), (0, 0), (1, 1)))
    flat = sum(resp[:, kx, :, :, kx : kx + cols] for kx in range(3))
    terms = sum(
        jnp.pad(flat[ky], ((0, 0), (2 - ky, ky), (0, 0))) for ky in range(3)
    )
    terms_all = lax.all_gather(terms, "slab", axis=0)
    full_rows = rows * slabs
    latent = sum(
        jnp.pad(terms_all[s], ((0, 0), (s * rows, full_rows - (s + 1) * rows), (0, 0)))
        for s in range(slabs)
    )[:, 1:-1] * latent_scale
    tokens = latent.reshape(outs, full_rows // 2, 2, cols // 2, 2).transpose(1, 3, 2, 4, 0)
    tokens = tokens.reshape(-1, 4 * outs)
    full = tokens.shape[0]
    count = full // slabs
    own = slab * count
    high = lax.reduce_precision(tokens, 8, 7)
    mid = lax.reduce_precision(tokens - high, 8, 7)
    low = tokens - high - mid
    split = jnp.concatenate([high, mid, low], 1).astype(jnp.bfloat16)
    start = jnp.dot(
        split, jnp.concatenate([embed_w] * 3, 0), preferred_element_type=jnp.float32
    )
    row = lax.dynamic_index_in_dim(mod_table, labels[0], 0, keepdims=False).astype(jnp.float32)
    gain = 1.0 + row[width:]
    mean = jnp.mean(start, -1, keepdims=True)
    cent = start - mean
    inv = lax.rsqrt(jnp.mean(cent * cent, -1, keepdims=True) + norm_eps)
    normed = cent * inv
    modded = (normed * gain + row[:width]).astype(jnp.bfloat16)

    def mine(whole):
        return lax.dynamic_slice_in_dim(whole, own, count, 0)

    kv = jnp.dot(modded, qkv_w[:, width:], preferred_element_type=jnp.float32).astype(jnp.bfloat16)
    query = jnp.dot(
        mine(modded), qkv_w[:, :width], preferred_element_type=jnp.float32
    ).astype(jnp.bfloat16)
    attended, lse = attend(query, kv)
    resid = mine(start) + jnp.dot(attended, out_w, preferred_element_type=jnp.float32)
    resid_b = resid.astype(jnp.bfloat16)
    projected = jnp.dot(resid_b, proj_w, preferred_element_type=jnp.float32)
    cosine, grad_p = cosine_grad(projected, dino[0].astype(jnp.float32))
    grad_pb = grad_p.astype(jnp.bfloat16)
    proj_part = contract_first(resid_b, grad_pb).astype(jnp.bfloat16)
    grad_proj = lax.psum(proj_part, ("slab", "img")).astype(jnp.float32)
    grad_resid = contract_last(grad_pb, proj_w)
    grad_att = contract_last(grad_resid.astype(jnp.bfloat16), out_w).astype(jnp.bfloat16)
    grad_query, grad_key, grad_value = attend_back(query, kv, grad_att, attended, lse)

    def norm_back(grad_mod, inv, normed):
        grad_norm = grad_mod * gain
        return inv * (
            grad_norm
            - jnp.mean(grad_norm, -1, keepdims=True)
            - normed * jnp.mean(grad_norm * normed, -1, keepdims=True)
        )

    grad_mod = contract_last(grad_key, qkv_w[:, width : 2 * width]) + contract_last(
        grad_value, qkv_w[:, 2 * width :]
    )
    spread = contract_last(embed_w, norm_back(grad_mod, inv, normed).astype(jnp.bfloat16))
    grad_own = grad_resid + norm_back(
        contract_last(grad_query, qkv_w[:, :width]), mine(inv), mine(normed)
    )
    spread_own = contract_last(embed_w, grad_own.astype(jnp.bfloat16))
    spread = spread + lax.dynamic_update_slice_in_dim(
        jnp.zeros_like(spread), spread_own, own, 1
    )
    grad_tokens = lax.psum(spread, "slab")
    grad_latent = grad_tokens.reshape(2, 2, outs, full_rows // 2, cols // 2)
    grad_latent = grad_latent.transpose(2, 3, 0, 4, 1).reshape(outs, full_rows, cols)
    grad_latent = (grad_latent * latent_scale).astype(jnp.bfloat16)
    grad_pad = lax.dynamic_slice_in_dim(
        jnp.pad(grad_latent, ((0, 0), (1, 1), (1, 1))), slab * rows, rows + 2, 1
    )
    views = jnp.concatenate(
        [
            grad_pad[:, 2 - ky : 2 - ky + rows, 2 - kx : 2 - kx + cols]
            for ky in range(3)
            for kx in range(3)
        ],
        0,
    ).reshape(9 * outs, rows * cols)
    grad_image = contract_first(views, taps).astype(jnp.bfloat16).reshape(1, rows, cols, chans)
    conv_part = mm(views, cells, ((1,), (0,)))
    loss_part = jnp.sum(1.0 - cosine)
    summed = reduce_small(
        jnp.concatenate([conv_part.reshape(-1), loss_part[None]]), slabs, images
    )
    grad_conv = summed[:-1].reshape(9, outs, chans).transpose(0, 2, 1)
    return (grad_image, grad_proj, grad_conv, summed[-1] / (slabs * images * count))


def solution(mesh):
    in_specs = (
        P("img", "slab", None, None),
        P("img"),
        P(),
        P(),
        P(),
        P(),
        P(),
        P(),
        P("img", "slab", None),
    )
    out_specs = (P("img", "slab", None, None), P(), P(), P())
    return jax.shard_map(local, mesh=mesh, in_specs=in_specs, out_specs=out_specs, check_vma=False)
```

```python
import functools
import math

import jax
import jax.numpy as jnp
from jax import lax
from jax.experimental import pallas as pl
from jax.experimental.pallas import tpu as pltpu
from jax.sharding import PartitionSpec as P

HEAD_DIM = 64
PAIR = 2 * HEAD_DIM

latent_scale = 0.18215
norm_eps = 1e-06
cosine_eps = 1e-06

MESH_ID = pl.DeviceIdType.MESH


def mm(left, right, dims, kind=jnp.float32):
    return lax.dot_general(left, right, (dims, ((), ())), preferred_element_type=kind)


def contract_first(left, right):
    return mm(left, right, ((0,), (0,)))


def contract_last(left, right):
    return mm(left, right, ((1,), (1,)))


def attend_kernel(q_ref, k_ref, v_ref, o_ref, lse_ref):
    scale = HEAD_DIM ** (-0.5)
    outs = []
    for h in range(2):
        cut = slice(h * HEAD_DIM, (h + 1) * HEAD_DIM)
        s = contract_last(k_ref[:, cut], q_ref[:, cut] * jnp.bfloat16(scale))
        top = jnp.max(s, 0, keepdims=True)
        e = jnp.exp(s - top)
        total = jnp.sum(e, 0, keepdims=True)
        o = contract_first(v_ref[:, cut], e.astype(jnp.bfloat16)) / total
        lse_ref[0, h : h + 1, :] = top + jnp.log(total)
        outs.append(o)
    o_ref[...] = jnp.concatenate(outs, 0).T.astype(jnp.bfloat16)


def attend_back_kernel(q_ref, k_ref, v_ref, g_ref, o_ref, lse_ref, gq_ref, gk_ref, gv_ref):
    scale = HEAD_DIM ** (-0.5)
    prod = (g_ref[...].astype(jnp.float32) * o_ref[...].astype(jnp.float32)).T
    gqs = []
    for h in range(2):
        cut = slice(h * HEAD_DIM, (h + 1) * HEAD_DIM)
        qs = q_ref[:, cut] * jnp.bfloat16(scale)
        k = k_ref[:, cut]
        g = g_ref[:, cut]
        delta = jnp.sum(prod[cut], 0, keepdims=True)
        p = jnp.exp(contract_last(k, qs) - lse_ref[0, h : h + 1, :])
        ds = (p * (contract_last(v_ref[:, cut], g) - delta)).astype(jnp.bfloat16)
        gk_ref[:, cut] = mm(ds, qs, ((1,), (0,))).astype(jnp.bfloat16)
        gv_ref[:, cut] = mm(p.astype(jnp.bfloat16), g, ((1,), (0,))).astype(jnp.bfloat16)
        gqs.append(contract_first(k, ds) * scale)
    gq_ref[...] = jnp.concatenate(gqs, 0).T.astype(jnp.bfloat16)


def attend(query, kv):
    count, width = query.shape
    full = kv.shape[0]
    pairs = width // PAIR
    cost = pl.CostEstimate(
        flops=4 * count * full * width, bytes_accessed=2 * (2 * full + 2 * count) * width,
        transcendentals=count * full * width // HEAD_DIM)
    return pl.pallas_call(
        attend_kernel,
        grid=(pairs,),
        in_specs=[
            pl.BlockSpec((count, PAIR), lambda i: (0, i)),
            pl.BlockSpec((full, PAIR), lambda i: (0, i)),
            pl.BlockSpec((full, PAIR), lambda i: (0, i + pairs)),
        ],
        out_specs=[
            pl.BlockSpec((count, PAIR), lambda i: (0, i)),
            pl.BlockSpec((1, 2, count), lambda i: (i, 0, 0)),
        ],
        out_shape=[
            jax.ShapeDtypeStruct((count, width), jnp.bfloat16),
            jax.ShapeDtypeStruct((pairs, 2, count), jnp.float32),
        ],
        cost_estimate=cost,
        name="attend",
    )(query, kv, kv)


def attend_back(query, kv, grad, attended, lse):
    count, width = query.shape
    full = kv.shape[0]
    pairs = width // PAIR
    cost = pl.CostEstimate(
        flops=10 * count * full * width, bytes_accessed=2 * (4 * full + 4 * count) * width,
        transcendentals=count * full * width // HEAD_DIM)
    small = pl.BlockSpec((count, PAIR), lambda i: (0, i))
    large = pl.BlockSpec((full, PAIR), lambda i: (0, i))
    return pl.pallas_call(
        attend_back_kernel,
        grid=(pairs,),
        in_specs=[
            small,
            large,
            pl.BlockSpec((full, PAIR), lambda i: (0, i + pairs)),
            small,
            small,
            pl.BlockSpec((1, 2, count), lambda i: (i, 0, 0)),
        ],
        out_specs=[small, large, large],
        out_shape=[
            jax.ShapeDtypeStruct((count, width), jnp.bfloat16),
            jax.ShapeDtypeStruct((full, width), jnp.bfloat16),
            jax.ShapeDtypeStruct((full, width), jnp.bfloat16),
        ],
        cost_estimate=cost,
        name="attend_back",
    )(query, kv, kv, grad, attended, lse)


def reduce_kernel(chips, images, *refs):
    size = (len(refs) - 8) // 5
    xs, outs, near, half, recv = (refs[i * size : (i + 1) * size] for i in range(5))
    send0, recv0, send1, recv1, send2, recv2, send3, recv3 = refs[5 * size :]
    slab = lax.axis_index("slab")
    image = lax.axis_index("img")
    core = lax.rem(slab, 2)
    me = (slab // 2) * images + image
    partner = {"slab": slab + 1 - 2 * core, "img": image}

    def spot(peer):
        return {"slab": (peer // images) * 2 + core, "img": lax.rem(peer, images)}

    def each(body):
        def run(step, _):
            body(lax.rem(me + step, chips))
            return 0

        lax.fori_loop(1, chips, run, 0)

    def copy(src, dst, send, recv_sem, device):
        return pltpu.make_async_remote_copy(
            src_ref=src, dst_ref=dst, send_sem=send, recv_sem=recv_sem,
            device_id=device, device_id_type=MESH_ID)

    barrier = pltpu.get_barrier_semaphore()
    pl.semaphore_signal(barrier, inc=1, device_id=partner, device_id_type=MESH_ID)
    each(
        lambda peer: pl.semaphore_signal(
            barrier, inc=1, device_id=spot(peer), device_id_type=MESH_ID
        )
    )
    pl.semaphore_wait(barrier, chips)

    first = [
        copy(xs[i].at[1 - core], near[i], send0.at[i], recv0.at[i], partner) for i in range(size)
    ]
    for c in first:
        c.start()
    for i in range(size):
        first[i].wait_recv()
        kind = half[i].dtype

        def add(j, _, i=i, kind=kind):
            both = xs[i][core, j].astype(jnp.float32) + near[i][j].astype(jnp.float32)
            half[i][j] = both.astype(kind)
            return 0

        lax.fori_loop(0, chips, add, 0)
        each(
            lambda peer, i=i: copy(
                half[i].at[peer], recv[i].at[me], send1.at[i, peer], recv1.at[i, me], spot(peer)
            ).start()
        )
    for i in range(size):
        each(
            lambda peer, i=i: copy(
                half[i].at[peer], recv[i].at[peer], send1.at[i, peer], recv1.at[i, peer],
                spot(peer),
            ).wait_recv()
        )
        total = lax.fori_loop(
            1,
            chips,
            lambda step, acc, i=i: acc + recv[i][lax.rem(me + step, chips)].astype(jnp.float32),
            half[i][me].astype(jnp.float32),
        )
        outs[i][core, me] = total.astype(outs[i].dtype)
        each(
            lambda peer, i=i: copy(
                outs[i].at[core, me], outs[i].at[core, me], send2.at[i, peer], recv2.at[i, me],
                spot(peer),
            ).start()
        )
    last = [
        copy(outs[i].at[core], outs[i].at[core], send3.at[i], recv3.at[i], partner)
        for i in range(size)
    ]
    for i in range(size):
        each(
            lambda peer, i=i: copy(
                outs[i].at[core, me], outs[i].at[core, peer], send2.at[i, peer],
                recv2.at[i, peer], spot(peer),
            ).wait_recv()
        )
        last[i].start()
    for i in range(size):
        first[i].wait_send()
        each(
            lambda peer, i=i: copy(
                half[i].at[peer], recv[i].at[me], send1.at[i, peer], recv1.at[i, me], spot(peer)
            ).wait_send()
        )
        each(
            lambda peer, i=i: copy(
                outs[i].at[core, me], outs[i].at[core, me], send2.at[i, peer], recv2.at[i, me],
                spot(peer),
            ).wait_send()
        )
        copy(
            outs[i].at[core], outs[i].at[1 - core], send3.at[i], recv3.at[i], partner
        ).wait_recv()
        last[i].wait_send()


def reduce_all(big, flat, slabs, images):
    chips = slabs * images // 2
    rows = math.ceil(flat.size / (2 * chips) / 1024) * 8
    cells = jnp.pad(flat, (0, 2 * chips * rows * 128 - flat.size))
    cells = cells.reshape(2, chips, rows, 128)
    parts = [big.reshape(2, chips, -1, big.shape[1]), cells]
    vmem = pl.BlockSpec(memory_space=pltpu.VMEM)
    shapes = [(p.shape, p.dtype) for p in parts]
    dma = pltpu.SemaphoreType.DMA
    out = pl.pallas_call(
        functools.partial(reduce_kernel, chips, images),
        out_shape=[jax.ShapeDtypeStruct(*s) for s in shapes],
        in_specs=[vmem] * 2,
        out_specs=[vmem] * 2,
        scratch_shapes=[pltpu.VMEM(s[1:], k) for s, k in shapes] * 3
        + [dma((2,))] * 2
        + [dma((2, chips))] * 4
        + [dma((2,))] * 2,
        compiler_params=pltpu.CompilerParams(collective_id=0, has_side_effects=True),
        name="reduce_all",
    )(*parts)
    return out[0].reshape(big.shape), out[1].reshape(-1)[: flat.size]


def cosine_grad(projected, target):
    norm_p = jnp.sqrt(jnp.sum(projected * projected, -1, keepdims=True) + cosine_eps)
    norm_t = jnp.sqrt(jnp.sum(target * target, -1, keepdims=True) + cosine_eps)
    cosine = jnp.sum(projected * target, -1, keepdims=True) / (norm_p * norm_t)
    grad = cosine * projected / (norm_p * norm_p) - target / (norm_p * norm_t)
    return (cosine[:, 0], grad)


def local(feats, labels, conv_w, embed_w, mod_table, qkv_w, out_w, proj_w, dino):
    image = feats[0]
    rows, cols, chans = image.shape
    outs = conv_w.shape[2]
    width = qkv_w.shape[0]
    slabs = lax.axis_size("slab")
    images = lax.axis_size("img")
    slab = lax.axis_index("slab")
    cells = image.reshape(rows * cols, chans)
    taps = conv_w.transpose(0, 2, 1).reshape(9 * outs, chans)
    resp = contract_last(taps, cells).reshape(3, 3, outs, rows, cols)
    resp = jnp.pad(resp, ((0, 0), (0, 0), (0, 0), (0, 0), (1, 1)))
    flat = sum(resp[:, kx, :, :, kx : kx + cols] for kx in range(3))
    terms = sum(
        jnp.pad(flat[ky], ((0, 0), (2 - ky, ky), (0, 0))) for ky in range(3)
    )
    terms_all = lax.all_gather(terms, "slab", axis=0)
    full_rows = rows * slabs
    latent = sum(
        jnp.pad(terms_all[s], ((0, 0), (s * rows, full_rows - (s + 1) * rows), (0, 0)))
        for s in range(slabs)
    )[:, 1:-1] * latent_scale
    tokens = latent.reshape(outs, full_rows // 2, 2, cols // 2, 2).transpose(1, 3, 2, 4, 0)
    tokens = tokens.reshape(-1, 4 * outs)
    full = tokens.shape[0]
    count = full // slabs
    own = slab * count
    high = lax.reduce_precision(tokens, 8, 7)
    mid = lax.reduce_precision(tokens - high, 8, 7)
    low = tokens - high - mid
    split = jnp.concatenate([high, mid, low], 1).astype(jnp.bfloat16)
    start = jnp.dot(
        split, jnp.concatenate([embed_w] * 3, 0), preferred_element_type=jnp.float32
    )
    row = lax.dynamic_index_in_dim(mod_table, labels[0], 0, keepdims=False).astype(jnp.float32)
    gain = 1.0 + row[width:]
    mean = jnp.mean(start, -1, keepdims=True)
    cent = start - mean
    inv = lax.rsqrt(jnp.mean(cent * cent, -1, keepdims=True) + norm_eps)
    normed = cent * inv
    modded = (normed * gain + row[:width]).astype(jnp.bfloat16)

    def mine(whole):
        return lax.dynamic_slice_in_dim(whole, own, count, 0)

    kv = jnp.dot(modded, qkv_w[:, width:], preferred_element_type=jnp.float32).astype(jnp.bfloat16)
    query = jnp.dot(
        mine(modded), qkv_w[:, :width], preferred_element_type=jnp.float32
    ).astype(jnp.bfloat16)
    attended, lse = attend(query, kv)
    resid = mine(start) + jnp.dot(attended, out_w, preferred_element_type=jnp.float32)
    resid_b = resid.astype(jnp.bfloat16)
    projected = jnp.dot(resid_b, proj_w, preferred_element_type=jnp.float32)
    cosine, grad_p = cosine_grad(projected, dino[0].astype(jnp.float32))
    grad_pb = grad_p.astype(jnp.bfloat16)
    proj_part = contract_first(resid_b, grad_pb).astype(jnp.bfloat16)
    grad_resid = contract_last(grad_pb, proj_w)
    grad_att = contract_last(grad_resid.astype(jnp.bfloat16), out_w).astype(jnp.bfloat16)
    grad_query, grad_key, grad_value = attend_back(query, kv, grad_att, attended, lse)

    def norm_back(grad_mod, inv, normed):
        grad_norm = grad_mod * gain
        return inv * (
            grad_norm
            - jnp.mean(grad_norm, -1, keepdims=True)
            - normed * jnp.mean(grad_norm * normed, -1, keepdims=True)
        )

    grad_mod = contract_last(grad_key, qkv_w[:, width : 2 * width]) + contract_last(
        grad_value, qkv_w[:, 2 * width :]
    )
    spread = contract_last(embed_w, norm_back(grad_mod, inv, normed).astype(jnp.bfloat16))
    grad_own = grad_resid + norm_back(
        contract_last(grad_query, qkv_w[:, :width]), mine(inv), mine(normed)
    )
    spread_own = contract_last(embed_w, grad_own.astype(jnp.bfloat16))
    spread = spread + lax.dynamic_update_slice_in_dim(
        jnp.zeros_like(spread), spread_own, own, 1
    )
    grad_tokens = jnp.sum(lax.all_gather(spread, "slab", axis=0), 0)
    grad_latent = grad_tokens.reshape(2, 2, outs, full_rows // 2, cols // 2)
    grad_latent = grad_latent.transpose(2, 3, 0, 4, 1).reshape(outs, full_rows, cols)
    grad_latent = (grad_latent * latent_scale).astype(jnp.bfloat16)
    grad_pad = lax.dynamic_slice_in_dim(
        jnp.pad(grad_latent, ((0, 0), (1, 1), (1, 1))), slab * rows, rows + 2, 1
    )
    views = jnp.concatenate(
        [
            grad_pad[:, 2 - ky : 2 - ky + rows, 2 - kx : 2 - kx + cols]
            for ky in range(3)
            for kx in range(3)
        ],
        0,
    ).reshape(9 * outs, rows * cols)
    grad_image = contract_first(views, taps).astype(jnp.bfloat16).reshape(1, rows, cols, chans)
    conv_part = mm(views, cells, ((1,), (0,)))
    loss_part = jnp.sum(1.0 - cosine)
    proj_sum, summed = reduce_all(
        proj_part, jnp.concatenate([conv_part.reshape(-1), loss_part[None]]), slabs, images
    )
    grad_proj = proj_sum.astype(jnp.float32)
    grad_conv = summed[:-1].reshape(9, outs, chans).transpose(0, 2, 1)
    return (grad_image, grad_proj, grad_conv, summed[-1] / (slabs * images * count))


def solution(mesh):
    in_specs = (
        P("img", "slab", None, None),
        P("img"),
        P(),
        P(),
        P(),
        P(),
        P(),
        P(),
        P("img", "slab", None),
    )
    out_specs = (P("img", "slab", None, None), P(), P(), P())
    return jax.shard_map(local, mesh=mesh, in_specs=in_specs, out_specs=out_specs, check_vma=False)
```
